32 devices in a mesh: dp: 4 (over y, core), row: 4 (over z), col: 2 (over x).
Axes of the slice: x: 2, y: 2, z: 4, core: 2. Of those that a mesh axis runs over, the one named last changes fastest.
Arguments:
- tokens: bfloat16 [8192, 2048], P(('dp', 'col'), 'row'), may hold values from -6 to 6
- gain_attn: bfloat16 [2048], P('row'), may hold values from 0.5 to 1.5
- w_query: bfloat16 [2048, 2048], P('row', 'col'), may hold values from -0.125 to 0.125
- w_key: bfloat16 [2048, 256], P('row', 'col'), may hold values from -0.125 to 0.125
- w_value: bfloat16 [2048, 256], P('row', 'col'), may hold values from -0.125 to 0.125
- w_out: bfloat16 [2048, 2048], P('col', 'row'), may hold values from -0.5 to 0.5
- gain_mlp: bfloat16 [2048], P('row'), may hold values from 0.5 to 1.5
- w_gate: bfloat16 [2048, 5632], P('row', 'col'), may hold values from -0.125 to 0.125
- w_up: bfloat16 [2048, 5632], P('row', 'col'), may hold values from -0.125 to 0.125
- w_down: bfloat16 [5632, 2048], P('col', 'row'), may hold values from -0.078125 to 0.078125
- segments: int32 [4, 2048], P('dp'), may hold values from 0 to 3, never falling along the last dimension, each value on 1 to 1536 neighbouring positions
- cotangent: bfloat16 [8192, 2048], P(('dp', 'col'), 'row'), may hold values from -6 to 6
Outputs:
- output: bfloat16 [8192, 2048], P(('dp', 'col'), 'row')
- input_grad: float32 [8192, 2048], P(('dp', 'col'), 'row')
- w_query_grad: float32 [2048, 2048], P(('row', 'dp'), 'col')
- w_key_grad: float32 [2048, 256], P(('row', 'dp'), 'col')
- w_value_grad: float32 [2048, 256], P(('row', 'dp'), 'col')
- w_out_grad: float32 [2048, 2048], P(('col', 'dp'), 'row')
- w_gate_grad: float32 [2048, 5632], P(('row', 'dp'), 'col')
- w_up_grad: float32 [2048, 5632], P(('row', 'dp'), 'col')
- w_down_grad: float32 [5632, 2048], P(('col', 'dp'), 'row')
- gain_attn_grad: float32 [2048], P(('row', 'dp'))
- gain_mlp_grad: float32 [2048], P(('row', 'dp'))
The draws below stay inside these ranges and needn't reach their ends.
Inputs may be any that keep to these rules, and one draw needn't show every extreme that they name: `segments`: segment numbers never fall along a sequence; a segment holds 1 to 1536 tokens and one holds exactly that many.
All inputs are finite; a program needn't handle non-finite values.
Results may differ from the reference program's by a relative error of at most 0.035.
Values may be sent and summed in bfloat16 or wider, within the bound.
A program may use at most 320 MiB of HBM per device.

```python
import math
import jax
import jax.numpy as jnp
import numpy as np
from jax import lax

D = 2048
HQ = 32
KV = 4
HD = 64
FF = 5632
SEQ = 2048
DOCS = 4
SEQS = 1
TOKENS = 8192
N_DP = 4


def steps_of(key, extent, pieces, least, top_value):
    def one(dim, shards_of):
        draws = jax.random.uniform(jax.random.fold_in(jax.random.fold_in(key, 6), dim), (shards_of,), jnp.float32, least / len(pieces), top_value / len(pieces))
        return jnp.repeat(jnp.exp(draws), extent[dim] // shards_of).reshape((-1,) + (1,) * (len(extent) - dim - 1))

    level = one(*pieces[0])
    for cut in pieces[1:]:
        level = level * one(*cut)
    return level


def profile(count, total, reach, lean):
    weights = [(1 << 20) // math.isqrt(grade ** lean) + 1 for grade in range(2, count + 1)]
    surplus, given = total - reach - (count - 1), [1] * (count - 1)
    while surplus > 0:
        free = [i for i in range(count - 1) if given[i] < reach]
        mass, left = sum([weights[i] for i in free]), surplus
        for i in free:
            addition = min(reach - given[i], max(1, left * weights[i] // mass), surplus)
            given[i] = given[i] + addition
            surplus = surplus - addition
    return np.array([reach] + given)


def uneven_parts(rng, number_of, total, most, skew):
    if number_of == 2:
        one = jax.random.randint(rng, (), max(1, total - most), min(most, total - 1) + 1)
        return jnp.stack([one, total - one])
    tallies = jnp.asarray(profile(number_of, total, most, skew), jnp.int32)
    twos = (number_of - 1) // 2
    source_of, sink = tallies[1:1 + 2 * twos:2], tallies[2:2 + 2 * twos:2]
    slack = jnp.minimum(source_of - 1, most - sink)
    passed = jax.random.randint(jax.random.fold_in(rng, 1), (twos,), 0, 1 << 20) % (slack + 1)
    tallies = tallies.at[1:1 + 2 * twos:2].set(source_of - passed).at[2:2 + 2 * twos:2].set(sink + passed)
    return tallies[jax.random.permutation(jax.random.fold_in(rng, 2), number_of)]


def scatter_about(rng, dims, width, reach, split=(), kind=jnp.bfloat16):
    entries = jax.random.normal(rng, dims, jnp.float32) * width
    if len(split) > 0:
        entries = steps_of(rng, dims, split, -0.22, 0.18) * entries
    return jnp.clip(entries, min=-reach, max=reach).astype(kind)


def setup_inputs(seed: int = 0) -> dict:
    key_list = jax.random.split(jax.random.key(seed), 13)
    tokens = scatter_about(key_list[0], (TOKENS, D), 1.0, 6.0, ((0, 8), (1, 4)))
    gain_attn = jnp.clip(1.0 + 0.1 * jax.random.normal(key_list[1], (D,), jnp.float32), 0.5, 1.5).astype(jnp.bfloat16)
    w_query = scatter_about(key_list[2], (D, HQ * HD), D ** -0.5, 0.125, ((0, 4), (1, 2)))
    w_key = scatter_about(key_list[3], (D, KV * HD), D ** -0.5, 0.125, ((0, 4), (1, 2)))
    w_value = scatter_about(key_list[4], (D, KV * HD), D ** -0.5, 0.125, ((0, 4), (1, 2)))
    w_out = scatter_about(key_list[5], (HQ * HD, D), (HQ * HD // 16) ** -0.5, 0.5, ((0, 2), (1, 4)))
    gain_mlp = jnp.clip(1.0 + 0.1 * jax.random.normal(key_list[6], (D,), jnp.float32), 0.5, 1.5).astype(jnp.bfloat16)
    w_gate = scatter_about(key_list[7], (D, FF), D ** -0.5, 0.125, ((0, 4), (1, 2)))
    w_up = scatter_about(key_list[8], (D, FF), D ** -0.5, 0.125, ((0, 4), (1, 2)))
    w_down = scatter_about(key_list[9], (FF, D), FF ** -0.5, 0.078125, ((0, 2), (1, 4)))
    segments = jax.vmap(lambda own: jnp.searchsorted(jnp.cumsum(uneven_parts(own, DOCS, SEQ, SEQ * 3 // 4, 0)), jnp.arange(SEQ), side="right"))(jax.random.split(key_list[10], (N_DP * SEQS))).reshape((N_DP * SEQS, SEQ)).astype(jnp.int32)
    cotangent = scatter_about(key_list[11], (TOKENS, D), 1.0, 6.0, ((0, 8), (1, 4)))
    return {"tokens": tokens, "gain_attn": gain_attn, "w_query": w_query, "w_key": w_key, "w_value": w_value, "w_out": w_out, "gain_mlp": gain_mlp, "w_gate": w_gate, "w_up": w_up, "w_down": w_down, "segments": segments, "cotangent": cotangent}


EPSILON = 1e-05
NEG_LARGE = -1e+30
HIGHEST = lax.Precision.HIGHEST

@jax.custom_vjp
def low(v):
    return lax.optimization_barrier(v.astype(jnp.bfloat16)).astype(jnp.float32)

@jax.custom_vjp
def low_back(v):
    return v

def low_keep(v):
    return (low(v), None)

def low_pass(kept, grad):
    return (grad,)

def back_keep(v):
    return (v, None)

def back_low(kept, grad):
    return (low(grad),)
low.defvjp(low_keep, low_pass)
low_back.defvjp(back_keep, back_low)

def positions_of(segments):
    seq_count, seq_length = segments.shape
    token_index = jnp.broadcast_to(jnp.arange(seq_length, dtype=jnp.int32)[None, :], (seq_count, seq_length))
    first_flag = jnp.concatenate([jnp.ones((seq_count, 1), dtype=bool), segments[:, 1:] != segments[:, :-1]], axis=1)
    begins = lax.cummax(jnp.where(first_flag, token_index, jnp.zeros_like(token_index)), axis=1)
    return (token_index - begins).astype(jnp.int32)

def rotate(values, cosine_table, sine_table):
    half_width = values.shape[-1] // 2
    first_half = values[..., :half_width]
    second_half = values[..., half_width:]
    cos_part = cosine_table[:, None, :]
    sin_part = sine_table[:, None, :]
    return jnp.concatenate([first_half * cos_part - second_half * sin_part, second_half * cos_part + first_half * sin_part], axis=-1)

def rms_norm(values, gain):
    inv_rms = lax.rsqrt(lax.optimization_barrier(jnp.mean(values * values, axis=-1, keepdims=True)) + EPSILON)
    return values * inv_rms * gain[None, :]

def product(left_side, right_side):
    return jnp.dot(left_side, right_side, precision=HIGHEST)

def attend_one(packed):
    queries, rotated_keys, values, segment_row = packed
    length = queries.shape[0]
    grouped = queries.reshape(length, KV, HQ // KV, HD)
    scores_now = low_back(jnp.einsum('qgpd,kgd->qgpk', grouped, rotated_keys, precision=HIGHEST) * HD ** (-0.5))
    token_index = jnp.arange(length, dtype=jnp.int32)
    visible_mask = (segment_row[:, None] == segment_row[None, :]) & (token_index[None, :] <= token_index[:, None])
    scores_now = jnp.where(visible_mask[:, None, None, :], scores_now, NEG_LARGE)
    probs = low(jax.nn.softmax(scores_now, axis=-1))
    return jnp.einsum('qgpk,kgd->qgpd', probs, values, precision=HIGHEST).reshape(length, HQ * HD)

def forward(inputs, gain_attn, w_query, w_key, w_value, w_out, gain_mlp, w_gate, w_up, w_down, cosine_table, sine_table, segments):
    seq_count, seq_length = segments.shape
    normed_attn = low(rms_norm(inputs, gain_attn))
    query_pre = low_back(product(normed_attn, w_query))
    key_pre = low_back(product(normed_attn, w_key))
    value_pre = low_back(product(normed_attn, w_value))
    queries = low(rotate(query_pre.reshape(-1, HQ, HD), cosine_table, sine_table))
    rotated_keys = low(rotate(key_pre.reshape(-1, KV, HD), cosine_table, sine_table))
    values = low(value_pre).reshape(-1, KV, HD)
    attended = lax.map(jax.checkpoint(attend_one), (queries.reshape(seq_count, seq_length, HQ, HD), rotated_keys.reshape(seq_count, seq_length, KV, HD), values.reshape(seq_count, seq_length, KV, HD), segments))
    attended = low(low_back(attended.reshape(-1, HQ * HD)))
    hidden_attn = inputs + low_back(product(attended, w_out))
    normed_mlp = low(rms_norm(hidden_attn, gain_mlp))
    gate_pre = low_back(product(normed_mlp, w_gate))
    up_pre = low_back(product(normed_mlp, w_up))
    hidden = low(jax.nn.silu(gate_pre) * up_pre)
    return hidden_attn + low_back(product(hidden, w_down))

def reference(tokens, gain_attn, w_query, w_key, w_value, w_out, gain_mlp, w_gate, w_up, w_down, segments, cotangent):
    seq_pos = positions_of(segments).reshape(-1)
    frequency = 10000.0 ** (-(jnp.arange(HD // 2, dtype=jnp.float32) * 2.0 / HD))
    angles = seq_pos.astype(jnp.float32)[:, None] * frequency[None, :]
    cosine_table = jnp.cos(angles)
    sine_table = jnp.sin(angles)

    def wrapped(inputs, gain_one, query_w, key_w, value_w, out_w, gain_two, gate_w, up_w, down_w):
        return forward(inputs, gain_one, query_w, key_w, value_w, out_w, gain_two, gate_w, up_w, down_w, cosine_table, sine_table, segments)
    output, pullback = jax.vjp(wrapped, tokens.astype(jnp.float32), gain_attn.astype(jnp.float32), w_query.astype(jnp.float32), w_key.astype(jnp.float32), w_value.astype(jnp.float32), w_out.astype(jnp.float32), gain_mlp.astype(jnp.float32), w_gate.astype(jnp.float32), w_up.astype(jnp.float32), w_down.astype(jnp.float32))
    grads = pullback(cotangent.astype(jnp.float32))
    return (output.astype(jnp.bfloat16), grads[0], grads[2], grads[3], grads[4], grads[5], grads[7], grads[8], grads[9], grads[1], grads[6])
```

```python
import jax
import jax.numpy as jnp
from jax import lax
from jax.sharding import PartitionSpec as P

D = 2048
HD = 64
EPSILON = 1e-05
NEG_LARGE = -1e30
BF = jnp.bfloat16
F32 = jnp.float32


def contract(left_side, right_side, left_dim, right_dim):
    return lax.dot_general(
        left_side,
        right_side,
        (((left_dim,), (right_dim,)), ((), ())),
        preferred_element_type=F32,
    )


def cat(parts, axis=0):
    return jnp.concatenate(parts, axis=axis)


def either(flag, first, second):
    return jnp.where(flag == 0, first, second)


def seg_positions(segments):
    seq_count, seq_length = segments.shape
    token_index = jnp.arange(seq_length, dtype=jnp.int32)[None, :]
    first_flag = jnp.concatenate(
        [jnp.ones((seq_count, 1), dtype=bool), segments[:, 1:] != segments[:, :-1]], axis=1
    )
    begins = lax.cummax(jnp.where(first_flag, token_index, jnp.zeros_like(token_index)), axis=1)
    return token_index - begins


def rotate(values, cosine_table, sine_table):
    half_width = values.shape[-1] // 2
    first_half = values[..., :half_width]
    second_half = values[..., half_width:]
    cos_part = cosine_table[:, None, :]
    sin_part = sine_table[:, None, :]
    return jnp.concatenate(
        [
            first_half * cos_part - second_half * sin_part,
            second_half * cos_part + first_half * sin_part,
        ],
        axis=-1,
    )


def rms_scale(values):
    return lax.rsqrt(jnp.sum(values * values, axis=1) / D + EPSILON)


def norm_back(grad_normed, values, inv_rms, gain):
    x_hat = values * inv_rms[:, None]
    upstream = grad_normed * gain[None, :]
    inner_sum = jnp.sum(upstream * x_hat, axis=1)
    grad_input = inv_rms[:, None] * (upstream - x_hat * (inner_sum / D)[:, None])
    return (grad_input, jnp.sum(grad_normed * x_hat, axis=0))


def shards(
    tokens,
    gain_attn,
    w_query,
    w_key,
    w_value,
    w_out,
    gain_mlp,
    w_gate,
    w_up,
    w_down,
    segments,
    cotangent,
):
    rows = lax.axis_size("row")
    dp_size = lax.axis_size("dp")
    spans = dp_size // 4
    assert lax.axis_size("col") == 2 and dp_size % 4 == 0 and segments.shape[0] == 1
    row_at = lax.axis_index("row")
    col_at = lax.axis_index("col")
    dp_at = lax.axis_index("dp")
    core_at = dp_at % 2
    y_at = (dp_at // 2) % 2
    token_half = tokens.shape[0]
    own_tokens = token_half // rows
    block = own_tokens // 2
    feat = tokens.shape[1]
    half_feat = feat // 2
    seq_length = segments.shape[1]
    wide = rows * half_feat

    swap_core = [(i, i ^ 1) for i in range(dp_size)]
    swap_y = [(i, i ^ 2) for i in range(dp_size)]

    def from_core(v):
        return lax.ppermute(v, "dp", swap_core)

    def from_y(v):
        return lax.ppermute(v, "dp", swap_y)

    def from_x(v):
        return lax.ppermute(v, "col", [(0, 1), (1, 0)])

    def own_y(v):
        parts = v.reshape((spans, 2, feat // (2 * spans)) + v.shape[1:])
        return lax.dynamic_index_in_dim(parts, y_at, 1, keepdims=False).reshape(
            (half_feat,) + v.shape[1:]
        )

    def y_order(v):
        parts = v.reshape(v.shape[0], spans, 2, feat // (2 * spans))
        low = parts[:, :, 0].reshape(v.shape[0], half_feat)
        high = parts[:, :, 1].reshape(v.shape[0], half_feat)
        return cat([either(y_at, low, high), either(y_at, high, low)], axis=1)

    def y_restore(v):
        own, other = v[:, :half_feat], v[:, half_feat:]
        low, high = either(y_at, own, other), either(y_at, other, own)
        shape = (v.shape[0], spans, 1, feat // (2 * spans))
        return cat([low.reshape(shape), high.reshape(shape)], axis=2).reshape(v.shape)

    def deal(v):
        parts = v.reshape(2, rows, block, v.shape[1])
        return jnp.stack([parts[0], parts[1, ::-1]], axis=1)

    def undeal(v):
        parts = v.reshape(rows, 2, block, v.shape[-1])
        return cat([parts[:, 0], parts[::-1, 1]]).reshape(token_half, v.shape[-1])

    def to_tokens(v):
        sent = deal(y_order(v)).reshape(rows, own_tokens, feat)
        came = lax.all_to_all(sent, "row", split_axis=0, concat_axis=0, tiled=True)
        came = came.reshape(rows, own_tokens, 2, half_feat)
        return came.transpose(1, 2, 0, 3).reshape(own_tokens, 2 * wide)

    def to_features(v):
        sent = v.astype(BF).reshape(own_tokens, 2, rows, half_feat)
        sent = sent.transpose(2, 0, 1, 3).reshape(rows, own_tokens, feat)
        came = lax.all_to_all(sent, "row", split_axis=0, concat_axis=0, tiled=True)
        return y_restore(undeal(came))

    def spread(v):
        across = from_x(v)
        return cat([v, across, from_core(v), from_core(across)])

    def fold(v):
        count = v.shape[0]
        summed = v[: count // 2] + from_core(v[count // 2 :].astype(BF)).astype(F32)
        return summed[: count // 4] + from_x(summed[count // 4 :].astype(BF)).astype(F32)

    def core_cols(v):
        parts = v.reshape(v.shape[0], 2, v.shape[1] // 2)
        return lax.dynamic_index_in_dim(parts, core_at, 1, keepdims=False)

    def core_rows(v):
        parts = v.reshape(2, v.shape[0] // 2, v.shape[1])
        return lax.dynamic_index_in_dim(parts, core_at, 0, keepdims=False)

    def fetch(piece):
        own = lax.all_gather(piece, "row", axis=0, tiled=True)
        return own, from_y(own)

    def ahead(left_side, weight):
        return contract(left_side[:, :wide], weight[0], 1, 0) + contract(
            left_side[:, wide:], weight[1], 1, 0
        )

    def back(left_side, weight):
        return cat(
            [contract(left_side, weight[0], 1, 1), contract(left_side, weight[1], 1, 1)], axis=1
        )

    def weight_grad(left_side, right_side):
        away = contract(left_side[:, wide:], right_side, 0, 0).astype(BF)
        kept = contract(left_side[:, :wide], right_side, 0, 0) + from_y(away).astype(F32)
        return lax.psum_scatter(kept.astype(BF), "row", scatter_dimension=0, tiled=True)

    span_groups = [[low + 4 * high for high in range(spans)] for low in range(4)]
    near_groups = [[4 * high + low for low in range(4)] for high in range(spans)]

    def finish_rows(tile):
        count = tile.shape[1]
        if spans > 1:
            tile = lax.psum_scatter(
                tile, "dp", scatter_dimension=0, tiled=True, axis_index_groups=span_groups
            )
        parts = tile.reshape(2, tile.shape[0] // 2, count)
        own = lax.dynamic_index_in_dim(parts, core_at, 0, keepdims=False)
        other = from_core(lax.dynamic_index_in_dim(parts, 1 - core_at, 0, keepdims=False))
        return lambda start, stop: cat(
            [
                either(core_at, own, other)[:, start:stop],
                either(core_at, other, own)[:, start:stop],
            ],
            axis=1,
        ).astype(F32)

    def finish_cols(tile):
        flipped = tile.T
        count = flipped.shape[0]
        if spans > 1:
            every = lax.all_gather(
                flipped, "dp", axis=0, tiled=False, axis_index_groups=near_groups
            ).reshape(2, 2, count, spans, half_feat // spans)
            whole = every.transpose(1, 2, 3, 0, 4).reshape(spans, 4, -1, feat)
            mine = lax.dynamic_index_in_dim(whole, dp_at % 4, 1, keepdims=False)
            return lax.psum_scatter(
                mine.reshape(-1, feat),
                "dp",
                scatter_dimension=0,
                tiled=True,
                axis_index_groups=span_groups,
            ).astype(F32)
        parts = flipped.reshape(2, count // 2, half_feat)
        same = lax.dynamic_index_in_dim(parts, y_at, 0, keepdims=False)
        cross = lax.dynamic_index_in_dim(parts, 1 - y_at, 0, keepdims=False)
        perm_same = [(2 * a + b, 2 * b + a) for a in range(2) for b in range(2)]
        perm_cross = [(2 * a + b, 2 * b + 1 - a) for a in range(2) for b in range(2)]
        first = lax.ppermute(same, "dp", perm_same)
        second = lax.ppermute(cross, "dp", perm_cross)
        return cat(
            [either(core_at, first, second), either(core_at, second, first)], axis=1
        ).astype(F32)

    query_width = w_query.shape[1] // 2
    key_width = w_key.shape[1] // 2
    ff_width = w_gate.shape[1] // 2
    heads = query_width // HD
    assert key_width == HD
    qkv_piece = cat(
        [core_cols(own_y(w_query)), core_cols(own_y(w_key)), core_cols(own_y(w_value))], axis=1
    )
    w_qkv = fetch(qkv_piece)
    w_out_t = fetch(own_y(core_rows(w_out).T))
    w_gate_b = fetch(core_cols(own_y(w_gate)))
    w_up_b = fetch(core_cols(own_y(w_up)))
    w_down_t = fetch(own_y(core_rows(w_down).T))

    both = cat([segments, from_core(segments)])
    placed = seg_positions(both)

    def dealt_index(row_index):
        cols = jnp.stack([col_at, 1 - col_at])[:, None] * (2 * rows)
        return (cols + jnp.stack([row_index, 2 * rows - 1 - row_index])[None, :]).reshape(-1)

    def picked(table, index):
        return table.reshape(2, 4 * rows, block)[:, index].reshape(2, -1)

    key_blocks = cat([dealt_index((row_at + j) % rows) for j in range(rows)])
    query_blocks = key_blocks[:4]
    spot = jnp.broadcast_to(jnp.arange(seq_length, dtype=jnp.int32)[None, :], (2, seq_length))
    query_spot, key_spot = picked(spot, query_blocks), picked(spot, key_blocks)
    query_seg, key_seg = picked(both, query_blocks), picked(both, key_blocks)
    query_pos = picked(placed, query_blocks).reshape(-1)
    frequency = 10000.0 ** (-(jnp.arange(HD // 2, dtype=F32) * 2.0 / HD))
    angles = query_pos.astype(F32)[:, None] * frequency[None, :]
    cosine_table = jnp.cos(angles)
    sine_table = jnp.sin(angles)
    score_scale = HD ** (-0.5)

    gains = lax.all_gather(
        y_order(jnp.stack([gain_attn, gain_mlp])).reshape(2, 2, half_feat), "row", axis=2
    ).reshape(2, 2 * wide)
    gain_one = gains[0].astype(F32)
    gain_two = gains[1].astype(F32)

    inputs = to_tokens(tokens).astype(F32)
    scale_attn = rms_scale(inputs)
    normed_attn = (inputs * scale_attn[:, None] * gain_one[None, :]).astype(BF)
    wide_attn = spread(normed_attn)
    count = wide_attn.shape[0]
    per_seq = count // 2
    qkv_pre = ahead(wide_attn, w_qkv)
    queries = (
        rotate(qkv_pre[:, :query_width].reshape(count, heads, HD), cosine_table, sine_table)
        .astype(BF)
        .reshape(2, per_seq, heads, HD)
    )
    keys_here = rotate(
        qkv_pre[:, query_width : query_width + HD].reshape(count, 1, HD), cosine_table, sine_table
    ).reshape(count, HD)
    kv_here = cat([keys_here, qkv_pre[:, query_width + HD :]], axis=1).astype(BF)

    def row_shift(j):
        return [(s, (s - j) % rows) for s in range(rows)]

    def row_return(j):
        return [(s, (s + j) % rows) for s in range(rows)]

    kv_all = jnp.stack(
        [kv_here.reshape(2, per_seq, 2 * HD)]
        + [
            lax.ppermute(kv_here, "row", row_shift(j)).reshape(2, per_seq, 2 * HD)
            for j in range(1, rows)
        ],
        axis=1,
    ).reshape(2, seq_length, 2 * HD)
    keys_all = kv_all[..., :HD]
    values_all = kv_all[..., HD:]
    visible = (
        (query_seg[:, :, None] == key_seg[:, None, :])
        & (key_spot[:, None, :] <= query_spot[:, :, None])
    )[:, :, None, :]

    def logits():
        raw = (
            jnp.einsum("bqhd,bkd->bqhk", queries, keys_all, preferred_element_type=F32)
            * score_scale
        )
        return jnp.where(visible, raw, NEG_LARGE)

    scores = logits()
    top = jnp.max(scores, axis=-1)
    exp_weight = jnp.where(visible, jnp.exp(scores - top[..., None]), 0.0)
    total = jnp.sum(exp_weight, axis=-1)
    attended_full = (
        jnp.einsum("bqhk,bkd->bqhd", exp_weight.astype(BF), values_all, preferred_element_type=F32)
        / total[..., None]
    )
    log_total = top + jnp.log(total)
    attended = attended_full.reshape(count, query_width).astype(BF)

    hidden_attn = inputs + fold(back(attended, w_out_t))
    scale_mlp = rms_scale(hidden_attn)
    normed_mlp = (hidden_attn * scale_mlp[:, None] * gain_two[None, :]).astype(BF)
    wide_mlp = spread(normed_mlp)
    gate_pre = ahead(wide_mlp, w_gate_b)
    up_pre = ahead(wide_mlp, w_up_b)
    sigmoid_gate = jax.nn.sigmoid(gate_pre)
    hidden = (gate_pre * sigmoid_gate * up_pre).astype(BF)
    output = to_features(hidden_attn + fold(back(hidden, w_down_t)))

    cot_tokens = to_tokens(cotangent)
    wide_cot = spread(cot_tokens)
    down_tile = weight_grad(wide_cot, hidden)
    grad_hidden = ahead(wide_cot, w_down_t)
    grad_gate = (
        grad_hidden * up_pre * sigmoid_gate * (1.0 + gate_pre * (1.0 - sigmoid_gate))
    ).astype(BF)
    grad_up = (grad_hidden * gate_pre * sigmoid_gate).astype(BF)
    gate_tile = weight_grad(wide_mlp, grad_gate)
    up_tile = weight_grad(wide_mlp, grad_up)
    grad_normed_mlp = fold(back(grad_gate, w_gate_b) + back(grad_up, w_up_b))
    grad_norm_two, gain_mlp_part = norm_back(grad_normed_mlp, hidden_attn, scale_mlp, gain_two)
    grad_resid = cot_tokens.astype(F32) + grad_norm_two
    wide_branch = spread(grad_resid.astype(BF))
    out_tile = weight_grad(wide_branch, attended)
    grad_attended = ahead(wide_branch, w_out_t).astype(BF).reshape(2, per_seq, heads, HD)
    delta = jnp.sum(grad_attended.astype(F32) * attended_full, axis=-1)

    probs = jnp.where(visible, jnp.exp(logits() - log_total[..., None]), 0.0)
    grad_probs = jnp.einsum(
        "bqhd,bkd->bqhk", grad_attended, values_all, preferred_element_type=F32
    )
    grad_scores = (probs * (grad_probs - delta[..., None])).astype(BF)
    grad_query = score_scale * jnp.einsum(
        "bqhk,bkd->bqhd", grad_scores, keys_all, preferred_element_type=F32
    )
    grad_keys_all = score_scale * jnp.einsum(
        "bqhk,bqhd->bkd", grad_scores, queries, preferred_element_type=F32
    )
    grad_values_all = jnp.einsum(
        "bqhk,bqhd->bkd", probs.astype(BF), grad_attended, preferred_element_type=F32
    )
    grad_kv = cat([grad_keys_all, grad_values_all], axis=2).reshape(2, rows, per_seq, 2 * HD)
    grad_kv_here = grad_kv[:, 0].reshape(count, 2 * HD)
    for j in range(1, rows):
        sent = grad_kv[:, j].reshape(count, 2 * HD).astype(BF)
        grad_kv_here = grad_kv_here + lax.ppermute(sent, "row", row_return(j)).astype(F32)
    grad_query_pre = rotate(
        grad_query.reshape(count, heads, HD), cosine_table, -sine_table
    ).reshape(count, query_width)
    grad_key_pre = rotate(
        grad_kv_here[:, :HD].reshape(count, 1, HD), cosine_table, -sine_table
    ).reshape(count, HD)
    grad_qkv = cat([grad_query_pre, grad_key_pre, grad_kv_here[:, HD:]], axis=1).astype(BF)
    qkv_tile = weight_grad(wide_attn, grad_qkv)
    grad_normed_attn = fold(back(grad_qkv, w_qkv))
    grad_norm_one, gain_attn_part = norm_back(grad_normed_attn, inputs, scale_attn, gain_one)
    input_grad = to_features(grad_resid + grad_norm_one).astype(F32)

    gain_sums = jnp.stack([gain_attn_part, gain_mlp_part]).reshape(2, 2, rows, half_feat)
    gain_sums = gain_sums.transpose(2, 0, 1, 3)
    gain_mine = lax.psum_scatter(gain_sums, "row", scatter_dimension=0, tiled=True)
    gain_rows = y_restore(gain_mine.reshape(2, feat))
    gain_rows = lax.psum(gain_rows, ("dp", "col")).reshape(2, dp_size, feat // dp_size)
    gain_out = lax.dynamic_index_in_dim(gain_rows, dp_at, 1, keepdims=False)

    qkv_part = finish_rows(qkv_tile)
    return (
        output,
        input_grad,
        qkv_part(0, query_width),
        qkv_part(query_width, query_width + HD),
        qkv_part(query_width + HD, query_width + 2 * HD),
        finish_cols(out_tile),
        finish_rows(gate_tile)(0, ff_width),
        finish_rows(up_tile)(0, ff_width),
        finish_cols(down_tile),
        gain_out[0],
        gain_out[1],
    )


def solution(mesh):
    placed = (
        P(("dp", "col"), "row"),
        P("row"),
        P("row", "col"),
        P("row", "col"),
        P("row", "col"),
        P("col", "row"),
        P("row"),
        P("row", "col"),
        P("row", "col"),
        P("col", "row"),
        P("dp", None),
        P(("dp", "col"), "row"),
    )
    return jax.shard_map(
        shards,
        mesh=mesh,
        in_specs=placed,
        out_specs=(
            P(("dp", "col"), "row"),
            P(("dp", "col"), "row"),
            P(("row", "dp"), "col"),
            P(("row", "dp"), "col"),
            P(("row", "dp"), "col"),
            P(("col", "dp"), "row"),
            P(("row", "dp"), "col"),
            P(("row", "dp"), "col"),
            P(("col", "dp"), "row"),
            P(("row", "dp")),
            P(("row", "dp")),
        ),
        check_vma=False,
    )
```

```python
import jax
import jax.numpy as jnp
from jax import lax
from jax.experimental import pallas as pl
from jax.experimental.pallas import tpu as pltpu
from jax.sharding import PartitionSpec as P

D = 2048
HD = 64
EPSILON = 1e-05
NEG_LARGE = -1e30
BF = jnp.bfloat16
F32 = jnp.float32


def contract(left_side, right_side, left_dim, right_dim):
    return lax.dot_general(
        left_side,
        right_side,
        (((left_dim,), (right_dim,)), ((), ())),
        preferred_element_type=F32,
    )


def cat(parts, axis=0):
    return jnp.concatenate(parts, axis=axis)


def either(flag, first, second):
    return jnp.where(flag == 0, first, second)


def seg_positions(segments):
    seq_count, seq_length = segments.shape
    token_index = jnp.arange(seq_length, dtype=jnp.int32)[None, :]
    first_flag = jnp.concatenate(
        [jnp.ones((seq_count, 1), dtype=bool), segments[:, 1:] != segments[:, :-1]], axis=1
    )
    begins = lax.cummax(jnp.where(first_flag, token_index, jnp.zeros_like(token_index)), axis=1)
    return token_index - begins


def lanes(shape):
    return lax.broadcasted_iota(jnp.int32, shape, 1)


def half_turn(v):
    low = lanes(v.shape) % HD < HD // 2
    return jnp.where(low, pltpu.roll(v, 2 * HD - HD // 2, 1), pltpu.roll(v, HD // 2, 1))


def bounds_mask(begin_row, block_at, step, block, heads):
    width = heads * block
    spot = lax.broadcasted_iota(jnp.int32, (2 * block, width), 0) + step * (2 * block)
    query = lax.broadcasted_iota(jnp.int32, (1, width), 1) % block + block_at * block
    begins = jnp.concatenate([begin_row] * heads, axis=1)
    return (spot >= begins) & (spot <= query)


def kernel_forward(low, high, canon, where, qkv, kv, cosine, sine, begin, out, queries, logsum):
    seq, part = pl.program_id(0), pl.program_id(1)
    block = out.shape[0]
    heads = out.shape[1] // HD
    width = heads * block
    left = lanes((block, 2 * HD)) < HD
    for pair in range(heads // 2):
        q = qkv[:, pair * 2 * HD : (pair + 1) * 2 * HD]
        q = (q * cosine[...] + half_turn(q) * sine[...]).astype(BF).astype(F32) * (HD**-0.5)
        queries[0, 2 * pair * block : (2 * pair + 1) * block] = jnp.where(left, q, 0.0).astype(BF)
        queries[0, (2 * pair + 1) * block : (2 * pair + 2) * block] = jnp.where(
            left, pltpu.roll(q, HD, 1), 0.0
        ).astype(BF)
    qz = queries[0]
    begin_row = begin[0, 0]
    block_at = canon[seq, part]

    def body(step, state):
        top, total, acc = state
        pair = jnp.concatenate([kv[0, where[2 * step]], kv[0, where[2 * step + 1]]], axis=0)
        scores = lax.dot_general(
            pair, qz, (((1,), (1,)), ((), ())), preferred_element_type=F32
        )
        scores = jnp.where(
            bounds_mask(begin_row, block_at, step, block, heads), scores, NEG_LARGE
        )
        new_top = jnp.maximum(top, jnp.max(scores, axis=0, keepdims=True))
        probs = jnp.exp(scores - new_top)
        shrink = jnp.exp(top - new_top)
        total = shrink * total + jnp.sum(probs, axis=0, keepdims=True)
        acc = shrink * acc + lax.dot_general(
            pair, probs.astype(BF), (((0,), (0,)), ((), ())), preferred_element_type=F32
        )
        return new_top, total, acc

    top, total, acc = lax.fori_loop(
        low[seq, part],
        high[seq, part],
        body,
        (
            jnp.full((1, width), NEG_LARGE, F32),
            jnp.zeros((1, width), F32),
            jnp.zeros((2 * HD, width), F32),
        ),
    )
    logsum[0, 0] = top + jnp.log(total)
    acc = acc / total
    for pair in range(heads // 2):
        even = acc[:, 2 * pair * block : (2 * pair + 1) * block].T
        odd = acc[:, (2 * pair + 1) * block : (2 * pair + 2) * block].T
        out[:, pair * 2 * HD : (pair + 1) * 2 * HD] = jnp.where(
            left, pltpu.roll(even, HD, 1), odd
        ).astype(BF)


def kernel_backward(
    low, high, canon, where, queries, kv, grad, attended, logsum, cosine, sine, begin,
    grad_query, grad_kv, grad_z, total_kv,
):
    seq, part = pl.program_id(0), pl.program_id(1)
    block = grad.shape[0]
    heads = grad.shape[1] // HD
    width = heads * block
    left = lanes((block, 2 * HD)) < HD

    @pl.when(part == 0)
    def _():
        total_kv[...] = jnp.zeros_like(total_kv)

    deltas = []
    for pair in range(heads // 2):
        cols = slice(pair * 2 * HD, (pair + 1) * 2 * HD)
        g = grad[:, cols].astype(F32)
        product = (g * attended[:, cols].astype(F32)).T
        deltas.append(jnp.sum(product[:HD], axis=0, keepdims=True))
        deltas.append(jnp.sum(product[HD:], axis=0, keepdims=True))
        grad_z[2 * pair * block : (2 * pair + 1) * block] = jnp.where(
            left, 0.0, pltpu.roll(g, HD, 1)
        ).astype(BF)
        grad_z[(2 * pair + 1) * block : (2 * pair + 2) * block] = jnp.where(left, 0.0, g).astype(BF)
    delta = jnp.concatenate(deltas, axis=1)
    qz = queries[0]
    gz = grad_z[...]
    level = logsum[0, 0]
    begin_row = begin[0, 0]
    block_at = canon[seq, part]

    def body(step, acc):
        first, second = where[2 * step], where[2 * step + 1]
        pair = jnp.concatenate([kv[0, first], kv[0, second]], axis=0)
        scores = lax.dot_general(
            pair, qz, (((1,), (1,)), ((), ())), preferred_element_type=F32
        )
        probs = jnp.where(
            bounds_mask(begin_row, block_at, step, block, heads), jnp.exp(scores - level), 0.0
        )
        grad_probs = lax.dot_general(
            pair, gz, (((1,), (1,)), ((), ())), preferred_element_type=F32
        )
        grad_scores = (probs * (grad_probs - delta)).astype(BF)
        both = jnp.dot(grad_scores, qz, preferred_element_type=F32) + jnp.dot(
            probs.astype(BF), gz, preferred_element_type=F32
        )
        total_kv[first] += both[:block]
        total_kv[second] += both[block:]
        return acc + lax.dot_general(
            pair, grad_scores, (((0,), (0,)), ((), ())), preferred_element_type=F32
        )

    acc = lax.fori_loop(
        low[seq, part], high[seq, part], body, jnp.zeros((2 * HD, width), F32)
    )
    acc = acc * (HD**-0.5)
    for pair in range(heads // 2):
        even = acc[:, 2 * pair * block : (2 * pair + 1) * block].T
        odd = acc[:, (2 * pair + 1) * block : (2 * pair + 2) * block].T
        q = jnp.where(left, even, pltpu.roll(odd, HD, 1))
        grad_query[:, pair * 2 * HD : (pair + 1) * 2 * HD] = (
            q * cosine[...] - half_turn(q) * sine[...]
        ).astype(BF)

    @pl.when(part == pl.num_programs(1) - 1)
    def _():
        grad_kv[0] = total_kv[...].astype(BF)


def attention_forward(tables, qkv, kv, cosine, sine, begin, query_width):
    count = qkv.shape[0]
    block = begin.shape[-1]
    parts = count // (2 * block)
    heads = query_width // HD
    width = heads * block

    def rows(s, p, *_):
        return (s * parts + p, 0)

    flops = 2 * count * heads * kv.shape[1] * block * 2 * HD
    return pl.pallas_call(
        kernel_forward,
        grid_spec=pltpu.PrefetchScalarGridSpec(
            num_scalar_prefetch=4,
            grid=(2, parts),
            in_specs=[
                pl.BlockSpec((block, qkv.shape[1]), rows),
                pl.BlockSpec((1,) + kv.shape[1:], lambda s, p, *_: (s, 0, 0, 0)),
                pl.BlockSpec((block, 2 * HD), rows),
                pl.BlockSpec((block, 2 * HD), rows),
                pl.BlockSpec((1, 1, 1, block), lambda s, p, *_: (s, p, 0, 0)),
            ],
            out_specs=[
                pl.BlockSpec((block, query_width), rows),
                pl.BlockSpec((1, width, 2 * HD), lambda s, p, *_: (s * parts + p, 0, 0)),
                pl.BlockSpec((1, 1, 1, width), lambda s, p, *_: (s, p, 0, 0)),
            ],
        ),
        out_shape=[
            jax.ShapeDtypeStruct((count, query_width), BF),
            jax.ShapeDtypeStruct((2 * parts, width, 2 * HD), BF),
            jax.ShapeDtypeStruct((2, parts, 1, width), F32),
        ],
        cost_estimate=pl.CostEstimate(
            flops=2 * flops, bytes_accessed=16 * count * query_width, transcendentals=0
        ),
        name="attention_forward",
    )(*tables, qkv, kv, cosine, sine, begin)


def attention_backward(tables, queries, kv, grad, attended, logsum, cosine, sine, begin):
    count, query_width = grad.shape
    block = begin.shape[-1]
    parts = count // (2 * block)
    heads = query_width // HD
    width = heads * block

    def rows(s, p, *_):
        return (s * parts + p, 0)

    flops = 2 * count * heads * kv.shape[1] * block * 2 * HD
    return pl.pallas_call(
        kernel_backward,
        grid_spec=pltpu.PrefetchScalarGridSpec(
            num_scalar_prefetch=4,
            grid=(2, parts),
            in_specs=[
                pl.BlockSpec((1, width, 2 * HD), lambda s, p, *_: (s * parts + p, 0, 0)),
                pl.BlockSpec((1,) + kv.shape[1:], lambda s, p, *_: (s, 0, 0, 0)),
                pl.BlockSpec((block, query_width), rows),
                pl.BlockSpec((block, query_width), rows),
                pl.BlockSpec((1, 1, 1, width), lambda s, p, *_: (s, p, 0, 0)),
                pl.BlockSpec((block, 2 * HD), rows),
                pl.BlockSpec((block, 2 * HD), rows),
                pl.BlockSpec((1, 1, 1, block), lambda s, p, *_: (s, p, 0, 0)),
            ],
            out_specs=[
                pl.BlockSpec((block, query_width), rows),
                pl.BlockSpec((1,) + kv.shape[1:], lambda s, p, *_: (s, 0, 0, 0)),
            ],
            scratch_shapes=[
                pltpu.VMEM((width, 2 * HD), BF),
                pltpu.VMEM(kv.shape[1:], F32),
            ],
        ),
        out_shape=[
            jax.ShapeDtypeStruct((count, query_width), BF),
            jax.ShapeDtypeStruct(kv.shape, BF),
        ],
        cost_estimate=pl.CostEstimate(
            flops=5 * flops, bytes_accessed=16 * count * query_width, transcendentals=0
        ),
        name="attention_backward",
    )(*tables, queries, kv, grad, attended, logsum, cosine, sine, begin)


def rms_scale(values):
    return lax.rsqrt(jnp.sum(values * values, axis=1) / D + EPSILON)


def norm_back(grad_normed, values, inv_rms, gain):
    x_hat = values * inv_rms[:, None]
    upstream = grad_normed * gain[None, :]
    inner_sum = jnp.sum(upstream * x_hat, axis=1)
    grad_input = inv_rms[:, None] * (upstream - x_hat * (inner_sum / D)[:, None])
    return (grad_input, jnp.sum(grad_normed * x_hat, axis=0))


def shards(
    tokens,
    gain_attn,
    w_query,
    w_key,
    w_value,
    w_out,
    gain_mlp,
    w_gate,
    w_up,
    w_down,
    segments,
    cotangent,
):
    rows = lax.axis_size("row")
    dp_size = lax.axis_size("dp")
    spans = dp_size // 4
    assert lax.axis_size("col") == 2 and dp_size % 4 == 0 and segments.shape[0] == 1
    row_at = lax.axis_index("row")
    col_at = lax.axis_index("col")
    dp_at = lax.axis_index("dp")
    core_at = dp_at % 2
    y_at = (dp_at // 2) % 2
    token_half = tokens.shape[0]
    own_tokens = token_half // rows
    block = own_tokens // 2
    feat = tokens.shape[1]
    half_feat = feat // 2
    seq_length = segments.shape[1]
    wide = rows * half_feat

    swap_core = [(i, i ^ 1) for i in range(dp_size)]
    swap_y = [(i, i ^ 2) for i in range(dp_size)]

    def from_core(v):
        return lax.ppermute(v, "dp", swap_core)

    def from_y(v):
        return lax.ppermute(v, "dp", swap_y)

    def from_x(v):
        return lax.ppermute(v, "col", [(0, 1), (1, 0)])

    def own_y(v):
        parts = v.reshape((spans, 2, feat // (2 * spans)) + v.shape[1:])
        return lax.dynamic_index_in_dim(parts, y_at, 1, keepdims=False).reshape(
            (half_feat,) + v.shape[1:]
        )

    def y_order(v):
        parts = v.reshape(v.shape[0], spans, 2, feat // (2 * spans))
        low = parts[:, :, 0].reshape(v.shape[0], half_feat)
        high = parts[:, :, 1].reshape(v.shape[0], half_feat)
        return cat([either(y_at, low, high), either(y_at, high, low)], axis=1)

    def y_restore(v):
        own, other = v[:, :half_feat], v[:, half_feat:]
        low, high = either(y_at, own, other), either(y_at, other, own)
        shape = (v.shape[0], spans, 1, feat // (2 * spans))
        return cat([low.reshape(shape), high.reshape(shape)], axis=2).reshape(v.shape)

    def deal(v):
        parts = v.reshape(2, rows, block, v.shape[1])
        return jnp.stack([parts[0], parts[1, ::-1]], axis=1)

    def undeal(v):
        parts = v.reshape(rows, 2, block, v.shape[-1])
        return cat([parts[:, 0], parts[::-1, 1]]).reshape(token_half, v.shape[-1])

    def to_tokens(v, extra=None):
        sent = deal(y_order(v)).reshape(rows, own_tokens, feat)
        if extra is not None:
            extra = y_order(extra)
            sent = cat([sent, jnp.broadcast_to(extra, (rows,) + extra.shape)], axis=1)
        came = lax.all_to_all(sent, "row", split_axis=0, concat_axis=0, tiled=True)
        came = came.reshape(rows, sent.shape[1], 2, half_feat)
        came = came.transpose(1, 2, 0, 3).reshape(sent.shape[1], 2 * wide)
        if extra is None:
            return came
        return came[:own_tokens], came[own_tokens:]

    def to_features(v):
        sent = v.astype(BF).reshape(own_tokens, 2, rows, half_feat)
        sent = sent.transpose(2, 0, 1, 3).reshape(rows, own_tokens, feat)
        came = lax.all_to_all(sent, "row", split_axis=0, concat_axis=0, tiled=True)
        return y_restore(undeal(came))

    def spread(v):
        across = from_x(v)
        return cat([v, across, from_core(v), from_core(across)])

    def fold(v):
        count = v.shape[0]
        summed = v[: count // 2] + from_core(v[count // 2 :].astype(BF)).astype(F32)
        return summed[: count // 4] + from_x(summed[count // 4 :].astype(BF)).astype(F32)

    def core_cols(v):
        parts = v.reshape(v.shape[0], 2, v.shape[1] // 2)
        return lax.dynamic_index_in_dim(parts, core_at, 1, keepdims=False)

    def core_rows(v):
        parts = v.reshape(2, v.shape[0] // 2, v.shape[1])
        return lax.dynamic_index_in_dim(parts, core_at, 0, keepdims=False)

    def fetch(piece):
        own = lax.all_gather(piece, "row", axis=0, tiled=True)
        return own, from_y(own)

    def ahead(left_side, weight):
        return contract(left_side[:, :wide], weight[0], 1, 0) + contract(
            left_side[:, wide:], weight[1], 1, 0
        )

    def back(left_side, weight):
        return cat(
            [contract(left_side, weight[0], 1, 1), contract(left_side, weight[1], 1, 1)], axis=1
        )

    def weight_grad(left_side, right_side):
        away = contract(left_side[:, wide:], right_side, 0, 0).astype(BF)
        kept = contract(left_side[:, :wide], right_side, 0, 0) + from_y(away).astype(F32)
        return lax.psum_scatter(kept.astype(BF), "row", scatter_dimension=0, tiled=True)

    span_groups = [[low + 4 * high for high in range(spans)] for low in range(4)]
    near_groups = [[4 * high + low for low in range(4)] for high in range(spans)]

    def finish_rows(tile):
        count = tile.shape[1]
        if spans > 1:
            tile = lax.psum_scatter(
                tile, "dp", scatter_dimension=0, tiled=True, axis_index_groups=span_groups
            )
        parts = tile.reshape(2, tile.shape[0] // 2, count)
        own = lax.dynamic_index_in_dim(parts, core_at, 0, keepdims=False)
        other = from_core(lax.dynamic_index_in_dim(parts, 1 - core_at, 0, keepdims=False))
        return lambda start, stop: cat(
            [
                either(core_at, own, other)[:, start:stop],
                either(core_at, other, own)[:, start:stop],
            ],
            axis=1,
        ).astype(F32)

    def finish_cols(tile):
        flipped = tile.T
        count = flipped.shape[0]
        if spans > 1:
            every = lax.all_gather(
                flipped, "dp", axis=0, tiled=False, axis_index_groups=near_groups
            ).reshape(2, 2, count, spans, half_feat // spans)
            whole = every.transpose(1, 2, 3, 0, 4).reshape(spans, 4, -1, feat)
            mine = lax.dynamic_index_in_dim(whole, dp_at % 4, 1, keepdims=False)
            return lax.psum_scatter(
                mine.reshape(-1, feat),
                "dp",
                scatter_dimension=0,
                tiled=True,
                axis_index_groups=span_groups,
            ).astype(F32)
        parts = flipped.reshape(2, count // 2, half_feat)
        same = lax.dynamic_index_in_dim(parts, y_at, 0, keepdims=False)
        cross = lax.dynamic_index_in_dim(parts, 1 - y_at, 0, keepdims=False)
        perm_same = [(2 * a + b, 2 * b + a) for a in range(2) for b in range(2)]
        perm_cross = [(2 * a + b, 2 * b + 1 - a) for a in range(2) for b in range(2)]
        first = lax.ppermute(same, "dp", perm_same)
        second = lax.ppermute(cross, "dp", perm_cross)
        return cat(
            [either(core_at, first, second), either(core_at, second, first)], axis=1
        ).astype(F32)

    query_width = w_query.shape[1] // 2
    key_width = w_key.shape[1] // 2
    ff_width = w_gate.shape[1] // 2
    assert key_width == HD
    qkv_piece = cat(
        [core_cols(own_y(w_query)), core_cols(own_y(w_key)), core_cols(own_y(w_value))], axis=1
    )
    w_qkv = fetch(qkv_piece)
    w_out_t = fetch(own_y(core_rows(w_out).T))
    w_gate_b = fetch(core_cols(own_y(w_gate)))
    w_up_b = fetch(core_cols(own_y(w_up)))
    w_down_t = fetch(own_y(core_rows(w_down).T))

    both = cat([segments, from_core(segments)])
    placed = seg_positions(both)
    blocks = 4 * rows

    def dealt_index(row_index):
        cols = jnp.stack([col_at, 1 - col_at])[:, None] * (2 * rows)
        return (cols + jnp.stack([row_index, 2 * rows - 1 - row_index])[None, :]).reshape(-1)

    key_blocks = cat([dealt_index((row_at + j) % rows) for j in range(rows)])
    query_blocks = key_blocks[:4]
    key_where = jnp.sum(
        jnp.where(
            key_blocks[None, :] == jnp.arange(blocks, dtype=jnp.int32)[:, None],
            jnp.arange(blocks, dtype=jnp.int32)[None, :],
            0,
        ),
        axis=1,
        dtype=jnp.int32,
    )
    query_placed = placed.reshape(2, blocks, block)[:, query_blocks]
    query_spot = query_blocks[:, None] * block + jnp.arange(block, dtype=jnp.int32)[None, :]
    query_begin = query_spot[None] - query_placed
    tables = (
        query_begin[:, :, 0] // (2 * block),
        jnp.broadcast_to((query_blocks // 2 + 1)[None, :], (2, 4)),
        jnp.broadcast_to(query_blocks[None, :], (2, 4)),
        key_where,
    )
    query_begin = query_begin[:, :, None, :]
    frequency = 10000.0 ** (-(jnp.arange(HD // 2, dtype=F32) * 2.0 / HD))
    angles = query_placed.reshape(-1).astype(F32)[:, None] * frequency[None, :]
    cos_part, sin_part = jnp.cos(angles), jnp.sin(angles)
    cosine = cat([cos_part] * 4, axis=1)
    sine = cat([-sin_part, sin_part, -sin_part, sin_part], axis=1)
    key_cosine = cat([cos_part, cos_part, jnp.ones_like(cosine[:, :HD])], axis=1)
    key_sine = cat([-sin_part, sin_part, jnp.zeros_like(cosine[:, :HD])], axis=1)

    def key_turn(v):
        return cat([v[:, HD // 2 : HD], v[:, : HD // 2], v[:, HD:]], axis=1)

    gain_rows = jnp.stack([gain_attn, gain_mlp])
    gain_rows = cat([gain_rows, jnp.zeros((14, feat), BF)])
    came, gains = to_tokens(tokens, gain_rows)
    inputs = came.astype(F32)
    gain_one = gains[0].astype(F32)
    gain_two = gains[1].astype(F32)
    scale_attn = rms_scale(inputs)
    normed_attn = (inputs * scale_attn[:, None] * gain_one[None, :]).astype(BF)
    wide_attn = spread(normed_attn)
    count = wide_attn.shape[0]
    per_seq = count // 2
    qkv_pre = ahead(wide_attn, w_qkv)
    kv_pre = qkv_pre[:, query_width:]
    kv_here = (kv_pre * key_cosine + key_turn(kv_pre) * key_sine).astype(BF)

    def row_shift(j):
        return [(s, (s - j) % rows) for s in range(rows)]

    def row_return(j):
        return [(s, (s + j) % rows) for s in range(rows)]

    kv_all = jnp.stack(
        [kv_here.reshape(2, per_seq, 2 * HD)]
        + [
            lax.ppermute(kv_here, "row", row_shift(j)).reshape(2, per_seq, 2 * HD)
            for j in range(1, rows)
        ],
        axis=1,
    ).reshape(2, blocks, block, 2 * HD)
    attended, queries, logsum = attention_forward(
        tables, qkv_pre, kv_all, cosine, sine, query_begin, query_width
    )

    hidden_attn = inputs + fold(back(attended, w_out_t))
    scale_mlp = rms_scale(hidden_attn)
    normed_mlp = (hidden_attn * scale_mlp[:, None] * gain_two[None, :]).astype(BF)
    wide_mlp = spread(normed_mlp)
    gate_pre = ahead(wide_mlp, w_gate_b)
    up_pre = ahead(wide_mlp, w_up_b)
    sigmoid_gate = jax.nn.sigmoid(gate_pre)
    hidden = (gate_pre * sigmoid_gate * up_pre).astype(BF)
    output = to_features(hidden_attn + fold(back(hidden, w_down_t)))

    cot_tokens = to_tokens(cotangent)
    wide_cot = spread(cot_tokens)
    down_tile = weight_grad(wide_cot, hidden)
    grad_hidden = ahead(wide_cot, w_down_t)
    grad_gate = (
        grad_hidden * up_pre * sigmoid_gate * (1.0 + gate_pre * (1.0 - sigmoid_gate))
    ).astype(BF)
    grad_up = (grad_hidden * gate_pre * sigmoid_gate).astype(BF)
    gate_tile = weight_grad(wide_mlp, grad_gate)
    up_tile = weight_grad(wide_mlp, grad_up)
    grad_normed_mlp = fold(back(grad_gate, w_gate_b) + back(grad_up, w_up_b))
    grad_norm_two, gain_mlp_part = norm_back(grad_normed_mlp, hidden_attn, scale_mlp, gain_two)
    grad_resid = cot_tokens.astype(F32) + grad_norm_two
    wide_branch = spread(grad_resid.astype(BF))
    out_tile = weight_grad(wide_branch, attended)
    grad_attended = ahead(wide_branch, w_out_t).astype(BF)
    grad_query_pre, grad_kv = attention_backward(
        tables, queries, kv_all, grad_attended, attended, logsum, cosine, sine, query_begin
    )
    grad_kv = grad_kv.reshape(2, rows, per_seq, 2 * HD)
    grad_kv_here = grad_kv[:, 0].reshape(count, 2 * HD).astype(F32)
    for j in range(1, rows):
        sent = grad_kv[:, j].reshape(count, 2 * HD)
        grad_kv_here = grad_kv_here + lax.ppermute(sent, "row", row_return(j)).astype(F32)
    grad_kv_pre = grad_kv_here * key_cosine - key_turn(grad_kv_here) * key_sine
    grad_qkv = cat([grad_query_pre, grad_kv_pre.astype(BF)], axis=1)
    qkv_tile = weight_grad(wide_attn, grad_qkv)
    grad_normed_attn = fold(back(grad_qkv, w_qkv))
    grad_norm_one, gain_attn_part = norm_back(grad_normed_attn, inputs, scale_attn, gain_one)
    input_grad = to_features(grad_resid + grad_norm_one).astype(F32)

    def gain_total(part):
        total = part.reshape(2, rows, half_feat)
        bit = 1
        while bit < dp_size:
            came = lax.ppermute(total, "dp", [(i, i ^ bit) for i in range(dp_size)])
            total = total + (came[::-1] if bit == 2 else came)
            bit *= 2
        total = total + from_x(total)
        mine = lax.dynamic_index_in_dim(total, row_at, 1, keepdims=False)
        for j in range(1, rows):
            there = lax.dynamic_index_in_dim(total, (row_at + j) % rows, 1, keepdims=False)
            mine = mine + lax.ppermute(there, "row", row_return(j))
        whole = y_restore(mine.reshape(1, feat)).reshape(dp_size, feat // dp_size)
        return lax.dynamic_index_in_dim(whole, dp_at, 0, keepdims=False)

    qkv_part = finish_rows(qkv_tile)
    return (
        output,
        input_grad,
        qkv_part(0, query_width),
        qkv_part(query_width, query_width + HD),
        qkv_part(query_width + HD, query_width + 2 * HD),
        finish_cols(out_tile),
        finish_rows(gate_tile)(0, ff_width),
        finish_rows(up_tile)(0, ff_width),
        finish_cols(down_tile),
        gain_total(gain_attn_part),
        gain_total(gain_mlp_part),
    )


def solution(mesh):
    placed = (
        P(("dp", "col"), "row"),
        P("row"),
        P("row", "col"),
        P("row", "col"),
        P("row", "col"),
        P("col", "row"),
        P("row"),
        P("row", "col"),
        P("row", "col"),
        P("col", "row"),
        P("dp", None),
        P(("dp", "col"), "row"),
    )
    return jax.shard_map(
        shards,
        mesh=mesh,
        in_specs=placed,
        out_specs=(
            P(("dp", "col"), "row"),
            P(("dp", "col"), "row"),
            P(("row", "dp"), "col"),
            P(("row", "dp"), "col"),
            P(("row", "dp"), "col"),
            P(("col", "dp"), "row"),
            P(("row", "dp"), "col"),
            P(("row", "dp"), "col"),
            P(("col", "dp"), "row"),
            P(("row", "dp")),
            P(("row", "dp")),
        ),
        check_vma=False,
    )
```
